128 devices in a mesh: dp: 32 (over x, y, core), mp: 4 (over z).
Axes of the slice: x: 4, y: 4, z: 4, core: 2. Of those that a mesh axis runs over, the one named last changes fastest.
Arguments:
- grad_parts: bfloat16 [32, 4, 1024, 4096], P('dp', None, None, 'mp'), may hold values from -4000 to 4000
- master: float32 [4, 1024, 4096], P(None, 'dp', 'mp'), may hold values from -6 to 6
- first_moment: float32 [4, 1024, 4096], P(None, 'dp', 'mp'), may hold values from -4 to 4
- second_moment: float32 [4, 1024, 4096], P(None, 'dp', 'mp'), may hold values from 0.25 to 4
- left_basis: bfloat16 [4, 1024, 4096], P(None, 'dp', 'mp'), may hold values from -1 to 1, as said below
- right_basis: bfloat16 [4, 1024, 4096], P(None, 'dp', 'mp'), may hold values from -1 to 1, as said below
Outputs:
- weights: bfloat16 [4, 1024, 4096], P(None, None, 'mp')
- new_master: float32 [4, 1024, 4096], P(None, 'dp', 'mp')
- new_first: float32 [4, 1024, 4096], P(None, 'dp', 'mp')
- new_second: float32 [4, 1024, 4096], P(None, 'dp', 'mp')
The draws below stay inside these ranges and needn't reach their ends.
Inputs may be any that keep to these rules, and one draw needn't show every extreme that they name: Each block left_basis[i, :, j * 1024 : (j + 1) * 1024] is an orthogonal 1024 x 1024 matrix up to rounding. Each block right_basis[i, :, j * 1024 : (j + 1) * 1024] is an orthogonal 1024 x 1024 matrix up to rounding.
All inputs are finite; a program needn't handle non-finite values.
Results may differ from the reference program's by a relative error of at most 0.02.
Values may be sent and summed in bfloat16 or wider, within the bound.
A program may use at most 128 MiB of HBM per device.

```python
import math
import jax
import jax.numpy as jnp
from jax import lax

D = 4096
BLK = 1024
STEP = 10
NB = 4
N_DP = 32


def orthogonal_blocks(key):
    block_count = D // BLK
    normal_part = jax.random.normal(key, (block_count, block_count, BLK, BLK), jnp.float32)
    factors = jnp.linalg.qr(normal_part)
    return factors[0].transpose(0, 2, 1, 3).reshape(block_count, BLK, D).astype(jnp.bfloat16)


def draw_left_basis(key, part):
    return orthogonal_blocks(jax.random.fold_in(key, 21))


def draw_right_basis(key, part):
    return orthogonal_blocks(jax.random.fold_in(key, 22))


def draw_grad_parts(key, part):
    subkeys = jax.random.split(jax.random.fold_in(key, 11), 5)
    places = jnp.arange(D, dtype=jnp.float32) / D
    row_scale = 10.0 ** (places + 0.3 * jax.random.uniform(subkeys[0], (D,), jnp.float32) - 0.15)
    column_scale = 10.0 ** (places + 0.3 * jax.random.uniform(subkeys[1], (D,), jnp.float32) - 0.15)
    normal_part = jax.random.normal(subkeys[4], (N_DP, D, D), jnp.float32)
    scaled = normal_part * row_scale[None, :, None] * column_scale[None, None, :]
    return scaled.reshape(N_DP, D // BLK, BLK, D).astype(jnp.bfloat16)


def level_of(stream_key, extent, cuts, least, top_value):
    factor_of = 1.0
    for position, blocks in cuts:
        steps = jax.random.uniform(jax.random.fold_in(jax.random.fold_in(stream_key, 6), position), (blocks,), jnp.float32, least / len(cuts), top_value / len(cuts))
        factor_of = factor_of * jnp.repeat(jnp.exp(steps), extent[position] // blocks).reshape((-1,) + (1,) * (len(extent) - 1 - position))
    return factor_of


def scatter_about(rng, shape, width, reach, cuts=(), held_as=jnp.bfloat16):
    entries = jax.random.normal(rng, shape, jnp.float32) * width
    if len(cuts) > 0:
        entries = level_of(rng, shape, cuts, -0.22, 0.18) * entries
    return jnp.clip(entries, min=-reach, max=reach).astype(held_as)


def setup_inputs(seed: int = 0) -> dict:
    splits = jax.random.split(jax.random.key(seed), 7)
    grad_parts = draw_grad_parts(jax.random.fold_in(splits[6], 71), 0)
    master = scatter_about(splits[1], (NB, BLK, D), 1.0, 6.0, ((1, 32), (2, 4)), jnp.float32)
    first_moment = scatter_about(splits[2], (NB, BLK, D), 0.5, 4.0, ((1, 32), (2, 4)), jnp.float32)
    second_moment = jnp.clip(jnp.exp(math.log(4.0) - 2.7725887 * jax.random.uniform(splits[3], (NB, BLK, D), jnp.float32) ** level_of(splits[3], (NB, BLK, D), ((1, 32), (2, 4)), -0.2, 0.2)), 0.25, 4.0)
    left_basis = draw_left_basis(jax.random.fold_in(splits[6], 71), 0)
    right_basis = draw_right_basis(jax.random.fold_in(splits[6], 71), 0)
    return dict(grad_parts=grad_parts, master=master, first_moment=first_moment, second_moment=second_moment, left_basis=left_basis, right_basis=right_basis)


beta_one = 0.95
beta_two = 0.95
epsilon = 1e-08
norm_epsilon = 1e-06
learning_rate = 0.3
decay_rate = 0.1

def reference(grad_parts, master, first_moment, second_moment, left_basis, right_basis):

    def add_part(running_sum, partial_value):
        return (running_sum + partial_value.astype(jnp.float32).reshape(D, D), None)
    gradient, unused_out = lax.scan(add_part, jnp.zeros((D, D), jnp.float32), grad_parts)
    squares_sum = jnp.sum(gradient * gradient)
    clip_scale = jnp.minimum(1.0, 2.0 * D / jnp.sqrt(squares_sum + norm_epsilon))
    grad_low = gradient.astype(jnp.bfloat16)
    master_flat = master.reshape(D, D)
    first_flat = first_moment.reshape(D, D)
    second_flat = second_moment.reshape(D, D)
    left_flat = left_basis.reshape(D, D)
    right_flat = right_basis.reshape(D, D)
    owner_rows = BLK // N_DP
    group_size = N_DP
    block_count = D // BLK
    bias_one = 1.0 - beta_one ** STEP
    bias_two = 1.0 - beta_two ** STEP
    master_rows, first_rows, second_rows = ([], [], [])
    for block_row in range(block_count):
        master_cols, first_cols, second_cols = ([], [], [])
        for block_column in range(block_count):
            row_span = slice(block_row * BLK, (block_row + 1) * BLK)
            column_span = slice(block_column * BLK, (block_column + 1) * BLK)
            grad_block = grad_low[row_span, column_span]
            left_block = left_flat[row_span, column_span]
            right_block = right_flat[row_span, column_span]
            turned = jnp.dot(grad_block.astype(jnp.float32), right_block.astype(jnp.float32), preferred_element_type=jnp.float32).astype(jnp.bfloat16)
            block_terms = jnp.einsum('gra,grb->gab', left_block.reshape(group_size, owner_rows, BLK).astype(jnp.float32), turned.reshape(group_size, owner_rows, BLK).astype(jnp.float32))
            rounded_terms = lax.optimization_barrier(block_terms.astype(jnp.bfloat16))
            rotated = lax.optimization_barrier(jnp.sum(rounded_terms.astype(jnp.float32), axis=0))
            clipped = clip_scale * rotated
            first_new = beta_one * first_flat[row_span, column_span] + (1.0 - beta_one) * clipped
            second_new = beta_two * second_flat[row_span, column_span] + (1.0 - beta_two) * clipped * clipped
            direction = (first_new / bias_one / (jnp.sqrt(second_new / bias_two) + epsilon)).astype(jnp.bfloat16)
            back_rows = jnp.dot(direction.astype(jnp.float32), right_block.T.astype(jnp.float32), preferred_element_type=jnp.float32).astype(jnp.bfloat16)
            update = jnp.dot(left_block.astype(jnp.float32), back_rows.astype(jnp.float32), preferred_element_type=jnp.float32)
            master_new = master_flat[row_span, column_span] * (1.0 - learning_rate * decay_rate) - learning_rate * update
            master_cols.append(master_new)
            first_cols.append(first_new)
            second_cols.append(second_new)
        master_rows.append(jnp.concatenate(master_cols, axis=1))
        first_rows.append(jnp.concatenate(first_cols, axis=1))
        second_rows.append(jnp.concatenate(second_cols, axis=1))
    new_master = jnp.concatenate(master_rows, axis=0).reshape(D // BLK, BLK, D)
    new_first = jnp.concatenate(first_rows, axis=0).reshape(D // BLK, BLK, D)
    new_second = jnp.concatenate(second_rows, axis=0).reshape(D // BLK, BLK, D)
    return (new_master.astype(jnp.bfloat16), new_master, new_first, new_second)
```

```python
import functools

import jax
import jax.numpy as jnp
from jax import lax
from jax.experimental import pallas as pl
from jax.experimental.pallas import tpu as pltpu
from jax.sharding import Mesh
from jax.sharding import PartitionSpec as P

D = 4096
STEP = 10
DP = ("dp_0", "dp_1", "dp_2")
MESH = pl.DeviceIdType.MESH

beta_one = 0.95
beta_two = 0.95
epsilon = 1e-08
norm_epsilon = 1e-06
learning_rate = 0.3
decay_rate = 0.1

F32 = jnp.float32
BF16 = jnp.bfloat16
N_SEMS = 160


def kernel(
    grad,
    master,
    first,
    second,
    left,
    right,
    weights,
    new_master,
    new_first,
    new_second,
    own,
    par,
    rec_a,
    rec_b,
    right_full,
    left_rows,
    left_cols,
    turned,
    back,
    states,
    states_out,
    master_in,
    first_in,
    second_in,
    grad_low,
    direction,
    rotated,
    rotated_out,
    rotated_in,
    update_out,
    update_in,
    squares,
    send_sems,
    recv_sems,
    local_sems,
):
    x, y, c, z = [lax.axis_index(n) for n in ("dp_0", "dp_1", "dp_2", "mp")]
    is_x = c == 0
    p_a = jnp.where(is_x, x, y)
    p_b = jnp.where(is_x, y, x)
    q = 2 * x + c
    h_own = y // 2

    def plus(v, d):
        return lax.rem(v + (d % 4), 4)

    def at_a(d):
        return (jnp.where(is_x, plus(x, d), x), jnp.where(is_x, y, plus(y, d)), c, z)

    def at_b(d):
        return (jnp.where(is_x, x, plus(x, d)), jnp.where(is_x, plus(y, d), y), c, z)

    def at_x(d):
        return (plus(x, d), y, c, z)

    partner = (x, y, 1 - c, z)
    used = [0]
    sent = []

    def sem_index():
        used[0] += 1
        return used[0] - 1

    def message(src, dst, device):
        k = sem_index()
        copy = pltpu.make_async_remote_copy(
            src_ref=src,
            dst_ref=dst,
            send_sem=send_sems.at[k],
            recv_sem=recv_sems.at[k],
            device_id=device,
            device_id_type=MESH,
        )
        copy.start()
        sent.append(copy)
        return copy

    barrier = pltpu.get_barrier_semaphore()
    peers = []
    for d in range(4):
        for e in range(2):
            if d or e:
                peers.append((plus(x, d), y, lax.rem(c + e, 2), z))
            if d:
                peers.append((x, plus(y, d), lax.rem(c + e, 2), z))
    for d in range(1, 4):
        peers.append((x, y, c, plus(z, d)))
    for device in peers:
        pl.semaphore_signal(barrier, inc=1, device_id=device, device_id_type=MESH)
    pl.semaphore_wait(barrier, len(peers))

    order_a = (2, 1, 3, 0)
    k_swap = [sem_index() for _ in range(4)]

    def slab_of(a, of_x):
        return grad.at[:, a, 0] if of_x else grad.at[a, :, 1]

    def swap_copy(n, a, of_x):
        return pltpu.make_async_remote_copy(
            src_ref=slab_of(a, of_x),
            dst_ref=par.at[a],
            send_sem=send_sems.at[k_swap[n]],
            recv_sem=recv_sems.at[k_swap[n]],
            device_id=partner,
            device_id_type=MESH,
        )

    for n, d in enumerate(order_a):
        for of_x in (True, False):

            @pl.when(is_x == of_x)
            def _():
                a = plus(x if of_x else y, d)
                pltpu.make_async_copy(slab_of(a, of_x), own.at[a], local_sems.at[n]).start()

            @pl.when(is_x != of_x)
            def _():
                swap_copy(n, plus(x if of_x else y, d), of_x).start()

    def wait_slab(n, d):
        a = plus(p_a, d)
        pltpu.make_async_copy(own.at[a], own.at[a], local_sems.at[n]).wait()
        pltpu.make_async_remote_copy(
            src_ref=par.at[a],
            dst_ref=par.at[a],
            send_sem=send_sems.at[k_swap[n]],
            recv_sem=recv_sems.at[k_swap[n]],
            device_id=partner,
            device_id_type=MESH,
        ).wait_recv()
        return a

    def add_slab(a):
        @pl.loop(0, 16)
        def _(t):
            b, r = t // 4, pl.multiple_of(lax.rem(t, 4) * 32, 32)
            rows = pl.ds(r, 32)
            own[a, b, rows, :] = own[a, b, rows, :] + par[a, b, rows, :]

    strip = 2 * lax.rem(y, 2) + c

    def to_block(pairs):
        k = [[sem_index() for _ in range(4)] for _ in pairs]
        for i in range(4):
            self_case = jnp.logical_and(y == i, c == h_own)
            for m, (source, place, whole) in enumerate(pairs):

                @pl.when(self_case)
                def _():
                    pltpu.make_async_copy(source(i), place, recv_sems.at[k[m][0]]).start()

                @pl.when(jnp.logical_not(self_case))
                def _():
                    pltpu.make_async_remote_copy(
                        src_ref=source(i),
                        dst_ref=place,
                        send_sem=send_sems.at[k[m][i]],
                        recv_sem=recv_sems.at[k[m][0]],
                        device_id=(x, jnp.int32(i), h_own, z),
                        device_id_type=MESH,
                    ).start()

        def wait_recv(m):
            whole = pairs[m][2]
            pltpu.make_async_copy(whole, whole, recv_sems.at[k[m][0]]).wait()

        def wait_send():
            for i in range(4):
                self_case = jnp.logical_and(y == i, c == h_own)

                @pl.when(jnp.logical_not(self_case))
                def _():
                    for m, (source, place, whole) in enumerate(pairs):
                        pltpu.make_async_remote_copy(
                            src_ref=source(i),
                            dst_ref=place,
                            send_sem=send_sems.at[k[m][i]],
                            recv_sem=recv_sems.at[k[m][0]],
                            device_id=(x, jnp.int32(i), h_own, z),
                            device_id_type=MESH,
                        ).wait_send()

        return wait_recv, wait_send

    place_rows = pl.ds(pl.multiple_of(strip * 32, 32), 32)
    bases_recv, bases_sent = to_block(
        [
            (lambda i: right.at[i], right_full.at[2 * x + h_own, place_rows], right_full.at[q]),
            (lambda i: left.at[i], left_rows.at[place_rows], left_rows),
        ]
    )
    for n, (source, place) in enumerate(
        ((master, master_in), (first, first_in), (second, second_in))
    ):
        pltpu.make_async_copy(source, place, local_sems.at[4 + n]).start()

    def to_owners(source, place, whole):
        k = [sem_index() for _ in range(4)]

        def case(s):
            yy, cc = 2 * c + s // 2, s % 2
            self_case = jnp.logical_and(yy == y, c == cc)
            copy = pltpu.make_async_remote_copy(
                src_ref=source.at[s],
                dst_ref=place.at[y],
                send_sem=send_sems.at[k[s]],
                recv_sem=recv_sems.at[k[0]],
                device_id=(x, yy, jnp.int32(cc), z),
                device_id_type=MESH,
            )
            return self_case, copy

        for s in range(4):
            self_case, copy = case(s)

            @pl.when(self_case)
            def _():
                pltpu.make_async_copy(source.at[s], place.at[y], recv_sems.at[k[0]]).start()

            @pl.when(jnp.logical_not(self_case))
            def _():
                copy.start()

        def wait_recv():
            pltpu.make_async_copy(whole, whole, recv_sems.at[k[0]]).wait()

        def wait_send():
            for s in range(4):
                self_case, copy = case(s)

                @pl.when(jnp.logical_not(self_case))
                def _():
                    copy.wait_send()

        return wait_recv, wait_send

    def half(ref, h):
        return ref.at[pl.ds(64 * h, 64)]

    class RowGather:
        def __init__(self, buf):
            self.buf = buf
            self.left = 2 * plus(x, -1) + c
            self.right = 2 * plus(x, 1) + c
            self.far = 2 * plus(x, 2) + c

        def start(self):
            mine = self.buf.at[q]
            self.from_left = message(mine, mine, at_x(1))
            self.from_right = message(mine, mine, at_x(-1))
            self.pair = [message(mine, mine, partner)]

        def forward_left(self):
            self.from_left.wait_recv()
            piece = self.buf.at[self.left]
            self.far_0 = message(half(piece, 0), half(piece, 0), at_x(1))
            self.pair.append(message(piece, piece, partner))

        def forward_right(self):
            self.from_right.wait_recv()
            piece = self.buf.at[self.right]
            self.far_1 = message(half(piece, 1), half(piece, 1), at_x(-1))
            self.pair.append(message(piece, piece, partner))

        def forward_far(self):
            self.far_0.wait_recv()
            self.far_1.wait_recv()
            piece = self.buf.at[self.far]
            self.pair.append(message(piece, piece, partner))

        def finish(self):
            for copy in self.pair:
                copy.wait_recv()

    b_of = [plus(p_b, d) for d in order_a]
    halves = (pl.ds(0, 64), pl.ds(64, 64))

    a_far, a_next, a_prev, a_own = [plus(p_a, d) for d in order_a]
    wait_slab(0, 2)
    add_slab(a_far)
    relay_r, relay_l = [], []
    for k in range(4):
        relay_r.append(message(own.at[a_far, b_of[k], halves[0]], rec_a.at[0, k], at_a(1)))
        relay_l.append(message(own.at[a_far, b_of[k], halves[1]], rec_a.at[1, k], at_a(-1)))
    wait_slab(1, 1)
    add_slab(a_next)
    direct_r = [
        message(own.at[a_next, b_of[k], halves[1]], rec_a.at[2, k], at_a(1)) for k in range(4)
    ]
    wait_slab(2, 3)
    add_slab(a_prev)
    direct_l = [
        message(own.at[a_prev, b_of[k], halves[0]], rec_a.at[3, k], at_a(-1)) for k in range(4)
    ]

    bases_recv(0)
    gather_right = RowGather(right_full)
    gather_right.start()
    bases_recv(1)
    mine = left_cols.at[q]
    tile_copies = []
    for d in range(4):
        for e in range(2):
            xx, cc = plus(x, d), lax.rem(c + e, 2)
            columns = pl.ds(pl.multiple_of((2 * xx + cc) * 128, 128), 128)
            if d or e:
                tile_copies.append(message(left_rows.at[:, columns], mine, (xx, y, cc, z)))
            else:
                own_tile = pltpu.make_async_copy(
                    left_rows.at[:, columns], mine, local_sems.at[7]
                )
                own_tile.start()

    wait_slab(3, 0)
    add_slab(a_own)

    final_r, final_l = [], []
    for k in range(4):
        relay_r[k].wait_recv()
        own[a_next, b_of[k], 0:64, :] = own[a_next, b_of[k], 0:64, :] + rec_a[0, k]
        final_r.append(message(own.at[a_next, b_of[k], halves[0]], rec_a.at[4, k], at_a(1)))
        relay_l[k].wait_recv()
        own[a_prev, b_of[k], 64:128, :] = own[a_prev, b_of[k], 64:128, :] + rec_a[1, k]
        final_l.append(message(own.at[a_prev, b_of[k], halves[1]], rec_a.at[5, k], at_a(-1)))

    gather_right.forward_left()
    gather_right.forward_right()

    for n, ref in enumerate((master_in, first_in, second_in)):
        pltpu.make_async_copy(ref, ref, local_sems.at[4 + n]).wait()

        @pl.loop(0, 4)
        def _(i):
            states_out[i, n] = ref[i].astype(BF16)

    def sum_first(k):
        direct_l[k].wait_recv()
        final_r[k].wait_recv()
        own[a_own, b_of[k], 0:64, :] = (
            own[a_own, b_of[k], 0:64, :].astype(F32)
            + rec_a[3, k].astype(F32)
            + rec_a[4, k].astype(F32)
        ).astype(BF16)
        direct_r[k].wait_recv()
        final_l[k].wait_recv()
        own[a_own, b_of[k], 64:128, :] = (
            own[a_own, b_of[k], 64:128, :].astype(F32)
            + rec_a[2, k].astype(F32)
            + rec_a[5, k].astype(F32)
        ).astype(BF16)

    sum_first(0)
    far = own.at[a_own, b_of[0]]
    second_relay_r = message(half(far, 0), rec_b.at[0], at_b(1))
    second_relay_l = message(half(far, 1), rec_b.at[1], at_b(-1))
    sum_first(1)
    second_direct_r = message(half(own.at[a_own, b_of[1]], 1), rec_b.at[2], at_b(1))
    sum_first(2)
    second_direct_l = message(half(own.at[a_own, b_of[2]], 0), rec_b.at[3], at_b(-1))
    second_relay_r.wait_recv()
    own[a_own, b_of[1], 0:64, :] = own[a_own, b_of[1], 0:64, :] + rec_b[0]
    second_final_r = message(half(own.at[a_own, b_of[1]], 0), rec_b.at[4], at_b(1))
    second_relay_l.wait_recv()
    own[a_own, b_of[2], 64:128, :] = own[a_own, b_of[2], 64:128, :] + rec_b[1]
    second_final_l = message(half(own.at[a_own, b_of[2]], 1), rec_b.at[5], at_b(-1))
    states_recv, states_sent = to_block(
        [(lambda i: states_out.at[i], states.at[strip], states)]
    )
    sum_first(3)
    gather_right.forward_far()

    def sum_second(rows, one, two):
        total = jnp.zeros((8, 1024), F32)
        for r in range(0, 64, 16):
            at = pl.ds(rows + r, 16)
            part = pl.ds(r, 16)
            value = (
                own[a_own, p_b, at, :].astype(F32)
                + rec_b[one, part, :].astype(F32)
                + rec_b[two, part, :].astype(F32)
            )
            grad_low[at, :] = value.astype(BF16)
            total = total + (value * value).reshape(2, 8, 1024).sum(0)
        return total

    second_direct_l.wait_recv()
    second_final_r.wait_recv()
    total = sum_second(0, 3, 4)
    second_direct_r.wait_recv()
    second_final_l.wait_recv()
    total = total + sum_second(64, 2, 5)
    total = total.reshape(8, 8, 128).sum(1) if False else sum(
        total[:, 128 * k : 128 * (k + 1)] for k in range(8)
    )
    squares[0] = total
    squares_pair = message(squares.at[0], squares.at[1], partner)

    gather_right.finish()
    for n in range(4):
        columns = slice(256 * n, 256 * (n + 1))
        acc = jnp.zeros((128, 256), F32)
        for k in range(8):
            acc = acc + jnp.dot(
                grad_low[:, 128 * k : 128 * (k + 1)],
                right_full[k, :, columns],
                preferred_element_type=F32,
            )
        turned[q, :, columns] = acc.astype(BF16)
    gather_turned = RowGather(turned)
    gather_turned.start()

    def spread_squares(slot, devices):
        return [
            message(squares.at[slot], squares.at[slot + 1 + n], device)
            for n, device in enumerate(devices)
        ]

    squares_pair.wait_recv()
    squares[2] = squares[0] + squares[1]
    over_x = spread_squares(2, [at_x(d) for d in (1, 2, 3)])
    gather_turned.forward_left()
    gather_turned.forward_right()
    for copy in over_x:
        copy.wait_recv()
    squares[6] = (squares[2] + squares[3]) + (squares[4] + squares[5])
    over_y = spread_squares(6, [(x, plus(y, d), c, z) for d in (1, 2, 3)])
    for copy in over_y:
        copy.wait_recv()
    squares[10] = (squares[6] + squares[7]) + (squares[8] + squares[9])
    over_z = spread_squares(10, [(x, y, c, plus(z, d)) for d in (1, 2, 3)])
    gather_turned.forward_far()
    for copy in over_z:
        copy.wait_recv()
    total = (squares[10] + squares[11]) + (squares[12] + squares[13])
    squares_sum = jnp.sum(jnp.sum(total, axis=1, keepdims=True), axis=0, keepdims=True)
    clip_scale = jnp.minimum(1.0, 2.0 * D / jnp.sqrt(squares_sum + norm_epsilon))

    own_tile.wait()
    for copy in tile_copies:
        copy.wait_recv()
    gather_turned.finish()
    states_recv(0)
    bias_one = 1.0 - beta_one**STEP
    bias_two = 1.0 - beta_two**STEP

    def moments(clipped, m, v):
        return (
            beta_one * m + (1.0 - beta_one) * clipped,
            beta_two * v + (1.0 - beta_two) * clipped * clipped,
        )

    for n in range(4):
        columns = slice(256 * n, 256 * (n + 1))
        acc = lax.dot_general(
            left_cols[...].reshape(1024, 128),
            turned[:, :, columns].reshape(1024, 256),
            (((0,), (0,)), ((), ())),
            preferred_element_type=F32,
        )
        for s in range(4):
            rows = acc[32 * s : 32 * (s + 1)]
            rotated_out[s, :, columns] = rows.astype(BF16)
            m, v = moments(
                clip_scale * rows,
                states[s, 1, :, columns].astype(F32),
                states[s, 2, :, columns].astype(F32),
            )
            direction[32 * s : 32 * (s + 1), columns] = (
                m / bias_one / (jnp.sqrt(v / bias_two) + epsilon)
            ).astype(BF16)

    for n in range(8):
        back[q, :, 128 * n : 128 * (n + 1)] = lax.dot_general(
            direction[...],
            right_full[n],
            (((1,), (1,)), ((), ())),
            preferred_element_type=F32,
        ).astype(BF16)
    gather_back = RowGather(back)
    gather_back.start()
    rotated_recv, rotated_sent = to_owners(rotated_out, rotated_in, rotated_in)
    gather_back.forward_left()
    gather_back.forward_right()

    rotated_recv()

    @pl.loop(0, 4)
    def _(i):
        m, v = moments(clip_scale * rotated_in[i].astype(F32), first_in[i], second_in[i])
        new_first[i] = m
        new_second[i] = v

    gather_back.forward_far()
    gather_back.finish()

    def piece(a, b):
        return weights.at[jnp.where(is_x, b, a), 2 * jnp.where(is_x, a, b) + c]

    keep = 1.0 - learning_rate * decay_rate
    for n in range(4):
        columns = slice(256 * n, 256 * (n + 1))
        acc = jnp.dot(
            left_rows[...],
            back[:, :, columns].reshape(1024, 256),
            preferred_element_type=F32,
        )
        for s in range(4):
            rows = acc[32 * s : 32 * (s + 1)]
            update_out[s, :, columns] = rows.astype(BF16)
            weights[y, q, 32 * s : 32 * (s + 1), columns] = (
                states[s, 0, :, columns].astype(F32) * keep - learning_rate * rows
            ).astype(BF16)

    pair = []

    def to_pair(ref):
        pair.append(message(ref, ref, partner))

    mine = piece(p_a, p_b)
    b_from_prev = message(mine, mine, at_b(1))
    b_from_next = message(mine, mine, at_b(-1))
    a_from_prev = [message(mine, mine, at_a(1))]
    a_from_next = [message(mine, mine, at_a(-1))]
    to_pair(mine)
    update_recv, update_sent = to_owners(update_out, update_in, update_in)

    b_from_prev.wait_recv()
    got = piece(p_a, plus(p_b, -1))
    b_far_0 = message(half(got, 0), half(got, 0), at_b(1))
    a_from_prev.append(message(got, got, at_a(1)))
    a_from_next.append(message(got, got, at_a(-1)))
    to_pair(got)
    b_from_next.wait_recv()
    got = piece(p_a, plus(p_b, 1))
    b_far_1 = message(half(got, 1), half(got, 1), at_b(-1))
    a_from_prev.append(message(got, got, at_a(1)))
    a_from_next.append(message(got, got, at_a(-1)))
    to_pair(got)
    a_far = []

    def pass_on(k, b):
        a_from_prev[k].wait_recv()
        got = piece(plus(p_a, -1), b)
        far_0 = message(half(got, 0), half(got, 0), at_a(1))
        to_pair(got)
        a_from_next[k].wait_recv()
        got = piece(plus(p_a, 1), b)
        far_1 = message(half(got, 1), half(got, 1), at_a(-1))
        to_pair(got)
        a_far.append((far_0, far_1, b))

    pass_on(0, p_b)
    b_far_0.wait_recv()
    b_far_1.wait_recv()
    got = piece(p_a, plus(p_b, 2))
    a_from_prev.append(message(got, got, at_a(1)))
    a_from_next.append(message(got, got, at_a(-1)))
    to_pair(got)

    update_recv()

    @pl.loop(0, 4)
    def _(i):
        new_master[i] = master_in[i] * keep - learning_rate * update_in[i].astype(F32)

    def take_far(k):
        far_0, far_1, b = a_far[k]
        far_0.wait_recv()
        far_1.wait_recv()
        to_pair(piece(plus(p_a, 2), b))

    pass_on(1, plus(p_b, -1))
    take_far(0)
    pass_on(2, plus(p_b, 1))
    take_far(1)
    pass_on(3, plus(p_b, 2))
    take_far(2)
    take_far(3)
    for copy in pair:
        copy.wait_recv()

    for copy in sent:
        copy.wait_send()
    for n, d in enumerate(order_a):
        swap_copy(n, d, False).wait_send()
    bases_sent()
    states_sent()
    rotated_sent()
    update_sent()


def per_device(grad_parts, master, first_moment, second_moment, left_basis, right_basis):
    vmem = pl.BlockSpec(memory_space=pltpu.VMEM)
    hbm = pl.BlockSpec(memory_space=pl.ANY)
    state = jax.ShapeDtypeStruct((4, 32, 1024), F32)
    weights, new_master, new_first, new_second = pl.pallas_call(
        kernel,
        out_shape=(
            jax.ShapeDtypeStruct((4, 8, 128, 1024), BF16),
            state,
            state,
            state,
        ),
        in_specs=[hbm] * 6,
        out_specs=(vmem, vmem, vmem, vmem),
        scratch_shapes=[
            pltpu.VMEM((4, 4, 128, 1024), BF16),
            pltpu.VMEM((4, 4, 128, 1024), BF16),
            pltpu.VMEM((6, 4, 64, 1024), BF16),
            pltpu.VMEM((6, 64, 1024), BF16),
            pltpu.VMEM((8, 128, 1024), BF16),
            pltpu.VMEM((128, 1024), BF16),
            pltpu.VMEM((8, 128, 128), BF16),
            pltpu.VMEM((8, 128, 1024), BF16),
            pltpu.VMEM((8, 128, 1024), BF16),
            pltpu.VMEM((4, 3, 32, 1024), BF16),
            pltpu.VMEM((4, 3, 32, 1024), BF16),
            pltpu.VMEM((4, 32, 1024), F32),
            pltpu.VMEM((4, 32, 1024), F32),
            pltpu.VMEM((4, 32, 1024), F32),
            pltpu.VMEM((128, 1024), BF16),
            pltpu.VMEM((128, 1024), BF16),
            pltpu.VMEM((128, 1024), F32),
            pltpu.VMEM((4, 32, 1024), BF16),
            pltpu.VMEM((4, 32, 1024), BF16),
            pltpu.VMEM((4, 32, 1024), BF16),
            pltpu.VMEM((4, 32, 1024), BF16),
            pltpu.VMEM((14, 8, 128), F32),
            pltpu.SemaphoreType.DMA((N_SEMS,)),
            pltpu.SemaphoreType.DMA((N_SEMS,)),
            pltpu.SemaphoreType.DMA((8,)),
        ],
        compiler_params=pltpu.CompilerParams(
            collective_id=0, has_side_effects=True, vmem_limit_bytes=60 * 1024 * 1024
        ),
    )(
        grad_parts.reshape(4, 4, 2, 128, 1024),
        master,
        first_moment,
        second_moment,
        left_basis,
        right_basis,
    )
    return (weights.reshape(4, 1024, 1024), new_master, new_first, new_second)


def solution(mesh):
    finer = Mesh(mesh.devices.reshape(4, 4, 2, mesh.shape["mp"]), ("dp_0", "dp_1", "dp_2", "mp"))
    placed = (
        P(DP, None, None, "mp"),
        P(None, DP, "mp"),
        P(None, DP, "mp"),
        P(None, DP, "mp"),
        P(None, DP, "mp"),
        P(None, DP, "mp"),
    )
    return jax.shard_map(
        per_device,
        mesh=finer,
        in_specs=placed,
        out_specs=(P(None, None, "mp"), P(None, DP, "mp"), P(None, DP, "mp"), P(None, DP, "mp")),
        check_vma=False,
    )
```

```python
import functools

import jax
import jax.numpy as jnp
from jax import lax
from jax.experimental import pallas as pl
from jax.experimental.pallas import tpu as pltpu
from jax.sharding import Mesh
from jax.sharding import PartitionSpec as P

D = 4096
STEP = 10
DP = ("dp_0", "dp_1", "dp_2")
MESH = pl.DeviceIdType.MESH

beta_one = 0.95
beta_two = 0.95
epsilon = 1e-08
norm_epsilon = 1e-06
learning_rate = 0.3
decay_rate = 0.1

F32 = jnp.float32
BF16 = jnp.bfloat16
N_SEMS = 200


def kernel(
    grad,
    master,
    first,
    second,
    left,
    right,
    weights,
    new_master,
    new_first,
    new_second,
    own,
    par,
    rec_a,
    rec_b,
    right_full,
    left_rows,
    left_cols,
    turned,
    back,
    moments_near,
    moments_out,
    master_near,
    master_out,
    master_in,
    first_in,
    second_in,
    grad_low,
    direction,
    rotated_out,
    rotated_in,
    update_out,
    update_in,
    squares,
    send_sems,
    recv_sems,
    local_sems,
):
    x, y, c, z = [lax.axis_index(n) for n in ("dp_0", "dp_1", "dp_2", "mp")]
    is_x = c == 0
    p_a = jnp.where(is_x, x, y)
    p_b = jnp.where(is_x, y, x)
    q = 2 * x + c
    h_own = y // 2

    def plus(v, d):
        return lax.rem(v + (d % 4), 4)

    def at_a(d):
        return (jnp.where(is_x, plus(x, d), x), jnp.where(is_x, y, plus(y, d)), c, z)

    def at_b(d):
        return (jnp.where(is_x, x, plus(x, d)), jnp.where(is_x, plus(y, d), y), c, z)

    def at_x(d):
        return (plus(x, d), y, c, z)

    partner = (x, y, 1 - c, z)
    used = [0]
    sent = []

    def sem_index():
        used[0] += 1
        return used[0] - 1

    def message(src, dst, device):
        k = sem_index()
        copy = pltpu.make_async_remote_copy(
            src_ref=src,
            dst_ref=dst,
            send_sem=send_sems.at[k],
            recv_sem=recv_sems.at[k],
            device_id=device,
            device_id_type=MESH,
        )
        copy.start()
        sent.append(copy)
        return copy

    order_a = (2, 1, 3, 0)
    k_swap = [sem_index() for _ in range(7)]
    blocks = [(0, k) for k in range(4)] + [(n, None) for n in (1, 2, 3)]

    def source_of(n, k, of_x):
        a = plus(x if of_x else y, order_a[n])
        if k is None:
            return (grad.at[:, a, 0] if of_x else grad.at[a, :, 1]), (a,)
        b = plus(y if of_x else x, order_a[k])
        return (grad.at[b, a, 0] if of_x else grad.at[a, b, 1]), (a, b)

    def swap_copy(m, of_x):
        source, place = source_of(*blocks[m], of_x)
        return pltpu.make_async_remote_copy(
            src_ref=source,
            dst_ref=par.at[place],
            send_sem=send_sems.at[k_swap[m]],
            recv_sem=recv_sems.at[k_swap[m]],
            device_id=partner,
            device_id_type=MESH,
        )

    for m in range(7):
        for of_x in (True, False):

            @pl.when(is_x == of_x)
            def _():
                source, place = source_of(*blocks[m], of_x)
                pltpu.make_async_copy(source, own.at[place], local_sems.at[m]).start()

    for n, (source, place) in enumerate(
        ((first, first_in), (second, second_in), (master, master_in))
    ):
        pltpu.make_async_copy(source, place, local_sems.at[7 + n]).start()

    barrier = pltpu.get_barrier_semaphore()
    peers = [partner]
    for d in range(1, 4):
        peers += [(plus(x, d), y, c, z), (plus(x, d), y, 1 - c, z)]
        peers += [(x, plus(y, d), c, z), (x, plus(y, d), 1 - c, z)]
        peers += [(x, y, c, plus(z, d))]
    for device in peers:
        pl.semaphore_signal(barrier, inc=1, device_id=device, device_id_type=MESH)
    pl.semaphore_wait(barrier, len(peers))

    for m in range(7):
        for of_x in (True, False):

            @pl.when(is_x != of_x)
            def _():
                swap_copy(m, of_x).start()

    def wait_part(m):
        n, k = blocks[m]
        a = plus(p_a, order_a[n])
        place = (a,) if k is None else (a, plus(p_b, order_a[k]))
        pltpu.make_async_copy(own.at[place], own.at[place], local_sems.at[m]).wait()
        pltpu.make_async_remote_copy(
            src_ref=par.at[place],
            dst_ref=par.at[place],
            send_sem=send_sems.at[k_swap[m]],
            recv_sem=recv_sems.at[k_swap[m]],
            device_id=partner,
            device_id_type=MESH,
        ).wait_recv()

    def add_part(a, b):
        @pl.loop(0, 4)
        def _(t):
            rows = pl.ds(pl.multiple_of(t * 32, 32), 32)
            own[a, b, rows, :] = own[a, b, rows, :] + par[a, b, rows, :]

    strip = 2 * lax.rem(y, 2) + c

    def to_block(source, place, whole):
        k = [sem_index() for _ in range(4)]

        def case(i):
            copy = pltpu.make_async_remote_copy(
                src_ref=source(i),
                dst_ref=place,
                send_sem=send_sems.at[k[i]],
                recv_sem=recv_sems.at[k[0]],
                device_id=(x, jnp.int32(i), h_own, z),
                device_id_type=MESH,
            )
            return jnp.logical_and(y == i, c == h_own), copy

        for i in range(4):
            self_case, copy = case(i)

            @pl.when(self_case)
            def _():
                pltpu.make_async_copy(source(i), place, recv_sems.at[k[0]]).start()

            @pl.when(jnp.logical_not(self_case))
            def _():
                copy.start()

        def wait_recv():
            pltpu.make_async_copy(whole, whole, recv_sems.at[k[0]]).wait()

        def wait_send():
            for i in range(4):
                self_case, copy = case(i)

                @pl.when(jnp.logical_not(self_case))
                def _():
                    copy.wait_send()

        return wait_recv, wait_send

    place_rows = pl.ds(pl.multiple_of(strip * 32, 32), 32)
    right_recv, right_sent = to_block(
        lambda i: right.at[i], right_full.at[2 * x + h_own, place_rows], right_full.at[q]
    )
    left_recv, left_sent = to_block(lambda i: left.at[i], left_rows.at[place_rows], left_rows)

    def to_owners(source, place, whole):
        k = [sem_index() for _ in range(4)]

        def case(s):
            yy, cc = 2 * c + s // 2, s % 2
            self_case = jnp.logical_and(yy == y, c == cc)
            copy = pltpu.make_async_remote_copy(
                src_ref=source.at[s],
                dst_ref=place.at[y],
                send_sem=send_sems.at[k[s]],
                recv_sem=recv_sems.at[k[0]],
                device_id=(x, yy, jnp.int32(cc), z),
                device_id_type=MESH,
            )
            return self_case, copy

        for s in range(4):
            self_case, copy = case(s)

            @pl.when(self_case)
            def _():
                pltpu.make_async_copy(source.at[s], place.at[y], recv_sems.at[k[0]]).start()

            @pl.when(jnp.logical_not(self_case))
            def _():
                copy.start()

        def wait_recv():
            pltpu.make_async_copy(whole, whole, recv_sems.at[k[0]]).wait()

        def wait_send():
            for s in range(4):
                self_case, copy = case(s)

                @pl.when(jnp.logical_not(self_case))
                def _():
                    copy.wait_send()

        return wait_recv, wait_send

    def half(ref, h):
        return ref.at[pl.ds(64 * h, 64)]

    class RowGather:
        def __init__(self, buf):
            self.left = buf.at[2 * plus(x, -1) + c]
            self.right = buf.at[2 * plus(x, 1) + c]
            self.far = buf.at[2 * plus(x, 2) + c]
            mine = buf.at[q]
            self.from_left = [message(half(mine, 0), half(mine, 0), at_x(1))]
            self.from_right = [message(half(mine, 1), half(mine, 1), at_x(-1))]
            self.from_left.append(message(half(mine, 1), half(mine, 1), at_x(1)))
            self.from_right.append(message(half(mine, 0), half(mine, 0), at_x(-1)))
            self.pair = [message(mine, mine, partner)]

        def pass_on(self):
            self.from_left[0].wait_recv()
            self.far_0 = message(half(self.left, 0), half(self.left, 0), at_x(1))
            self.from_right[0].wait_recv()
            self.far_1 = message(half(self.right, 1), half(self.right, 1), at_x(-1))

        def share(self):
            self.from_left[1].wait_recv()
            self.pair.append(message(self.left, self.left, partner))
            self.from_right[1].wait_recv()
            self.pair.append(message(self.right, self.right, partner))

        def share_far(self):
            self.far_0.wait_recv()
            self.pair.append(message(half(self.far, 0), half(self.far, 0), partner))
            self.far_1.wait_recv()
            self.pair.append(message(half(self.far, 1), half(self.far, 1), partner))

        def finish(self):
            for copy in self.pair:
                copy.wait_recv()

    b_of = [plus(p_b, d) for d in order_a]
    halves = (pl.ds(0, 64), pl.ds(64, 64))

    a_far, a_next, a_prev, a_own = [plus(p_a, d) for d in order_a]
    relay_r, relay_l = [], []
    for k in range(4):
        wait_part(k)
        add_part(a_far, b_of[k])
        relay_r.append(message(own.at[a_far, b_of[k], halves[0]], rec_a.at[0, k], at_a(1)))
        relay_l.append(message(own.at[a_far, b_of[k], halves[1]], rec_a.at[1, k], at_a(-1)))
    right_recv()
    gather_right = RowGather(right_full)
    wait_part(4)
    direct_r, direct_l = [], []
    for k in range(4):
        add_part(a_next, b_of[k])
        direct_r.append(message(own.at[a_next, b_of[k], halves[1]], rec_a.at[2, k], at_a(1)))
    wait_part(5)
    for k in range(4):
        add_part(a_prev, b_of[k])
        direct_l.append(message(own.at[a_prev, b_of[k], halves[0]], rec_a.at[3, k], at_a(-1)))
    left_recv()
    mine = left_cols.at[q]
    tile_copies = []
    for d in range(4):
        for e in range(2):
            xx, cc = plus(x, d), lax.rem(c + e, 2)
            columns = pl.ds(pl.multiple_of((2 * xx + cc) * 128, 128), 128)
            if d or e:
                tile_copies.append(message(left_rows.at[:, columns], mine, (xx, y, cc, z)))
            else:
                own_tile = pltpu.make_async_copy(
                    left_rows.at[:, columns], mine, local_sems.at[10]
                )
                own_tile.start()

    wait_part(6)
    for k in range(4):
        add_part(a_own, b_of[k])

    final_r, final_l = [], []
    for k in range(4):
        relay_r[k].wait_recv()
        own[a_next, b_of[k], 0:64, :] = own[a_next, b_of[k], 0:64, :] + rec_a[0, k]
        final_r.append(message(own.at[a_next, b_of[k], halves[0]], rec_a.at[4, k], at_a(1)))
        relay_l[k].wait_recv()
        own[a_prev, b_of[k], 64:128, :] = own[a_prev, b_of[k], 64:128, :] + rec_a[1, k]
        final_l.append(message(own.at[a_prev, b_of[k], halves[1]], rec_a.at[5, k], at_a(-1)))

    gather_right.pass_on()
    gather_right.share()

    for n, (ref, packed, m) in enumerate(
        ((first_in, moments_out, 0), (second_in, moments_out, 1), (master_in, master_out, None))
    ):
        pltpu.make_async_copy(ref, ref, local_sems.at[7 + n]).wait()

        @pl.loop(0, 4)
        def _(i):
            if m is None:
                packed[i] = ref[i].astype(BF16)
            else:
                packed[i, m] = ref[i].astype(BF16)

    def sum_first(k):
        direct_l[k].wait_recv()
        final_r[k].wait_recv()
        own[a_own, b_of[k], 0:64, :] = (
            own[a_own, b_of[k], 0:64, :].astype(F32)
            + rec_a[3, k].astype(F32)
            + rec_a[4, k].astype(F32)
        ).astype(BF16)
        direct_r[k].wait_recv()
        final_l[k].wait_recv()
        own[a_own, b_of[k], 64:128, :] = (
            own[a_own, b_of[k], 64:128, :].astype(F32)
            + rec_a[2, k].astype(F32)
            + rec_a[5, k].astype(F32)
        ).astype(BF16)

    sum_first(0)
    far = own.at[a_own, b_of[0]]
    second_relay_r = message(half(far, 0), rec_b.at[0], at_b(1))
    second_relay_l = message(half(far, 1), rec_b.at[1], at_b(-1))
    sum_first(1)
    second_direct_r = message(half(own.at[a_own, b_of[1]], 1), rec_b.at[2], at_b(1))
    sum_first(2)
    second_direct_l = message(half(own.at[a_own, b_of[2]], 0), rec_b.at[3], at_b(-1))
    second_relay_r.wait_recv()
    own[a_own, b_of[1], 0:64, :] = own[a_own, b_of[1], 0:64, :] + rec_b[0]
    second_final_r = message(half(own.at[a_own, b_of[1]], 0), rec_b.at[4], at_b(1))
    second_relay_l.wait_recv()
    own[a_own, b_of[2], 64:128, :] = own[a_own, b_of[2], 64:128, :] + rec_b[1]
    second_final_l = message(half(own.at[a_own, b_of[2]], 1), rec_b.at[5], at_b(-1))
    moments_recv, moments_sent = to_block(
        lambda i: moments_out.at[i], moments_near.at[strip], moments_near
    )
    sum_first(3)
    gather_right.share_far()

    def sum_second(rows, one, two):
        total = jnp.zeros((8, 1024), F32)
        for r in range(0, 64, 16):
            at = pl.ds(rows + r, 16)
            part = pl.ds(r, 16)
            value = (
                own[a_own, p_b, at, :].astype(F32)
                + rec_b[one, part, :].astype(F32)
                + rec_b[two, part, :].astype(F32)
            )
            grad_low[at, :] = value.astype(BF16)
            total = total + (value * value).reshape(2, 8, 1024).sum(0)
        return total

    second_direct_l.wait_recv()
    second_final_r.wait_recv()
    total = sum_second(0, 3, 4)
    second_direct_r.wait_recv()
    second_final_l.wait_recv()
    total = total + sum_second(64, 2, 5)
    squares[0] = sum(total[:, 128 * k : 128 * (k + 1)] for k in range(8))
    over_row = [message(squares.at[0], squares.at[1], partner)]
    for d in (1, 2, 3):
        for cc in (c, 1 - c):
            place = squares.at[len(over_row) + 1]
            over_row.append(message(squares.at[0], place, (plus(x, d), y, cc, z)))

    gather_right.finish()
    for n in range(4):
        columns = slice(256 * n, 256 * (n + 1))
        acc = jnp.zeros((128, 256), F32)
        for k in range(8):
            acc = acc + jnp.dot(
                grad_low[:, 128 * k : 128 * (k + 1)],
                right_full[k, :, columns],
                preferred_element_type=F32,
            )
        turned[q, :, columns] = acc.astype(BF16)
    gather_turned = RowGather(turned)
    for copy in over_row:
        copy.wait_recv()
    squares[8] = sum(squares[n] for n in range(8))
    over_y = [
        message(squares.at[8], squares.at[8 + d], (x, plus(y, d), c, z)) for d in (1, 2, 3)
    ]
    master_recv, master_sent = to_block(
        lambda i: master_out.at[i], master_near.at[strip], master_near
    )
    gather_turned.pass_on()
    for copy in over_y:
        copy.wait_recv()
    squares[12] = sum(squares[n] for n in range(8, 12))
    over_z = [
        message(squares.at[12], squares.at[12 + d], (x, y, c, plus(z, d))) for d in (1, 2, 3)
    ]
    gather_turned.share()
    gather_turned.share_far()
    for copy in over_z:
        copy.wait_recv()
    total = sum(squares[n] for n in range(12, 16))
    squares_sum = jnp.sum(jnp.sum(total, axis=1, keepdims=True), axis=0, keepdims=True)
    clip_scale = jnp.minimum(1.0, 2.0 * D / jnp.sqrt(squares_sum + norm_epsilon))

    own_tile.wait()
    for copy in tile_copies:
        copy.wait_recv()
    gather_turned.finish()
    moments_recv()
    bias_one = 1.0 - beta_one**STEP
    bias_two = 1.0 - beta_two**STEP

    def moments(clipped, m, v):
        return (
            beta_one * m + (1.0 - beta_one) * clipped,
            beta_two * v + (1.0 - beta_two) * clipped * clipped,
        )

    for n in range(4):
        columns = slice(256 * n, 256 * (n + 1))
        acc = lax.dot_general(
            left_cols[...].reshape(1024, 128),
            turned[:, :, columns].reshape(1024, 256),
            (((0,), (0,)), ((), ())),
            preferred_element_type=F32,
        )
        for s in range(4):
            rows = acc[32 * s : 32 * (s + 1)]
            rotated_out[s, :, columns] = rows.astype(BF16)
            m, v = moments(
                clip_scale * rows,
                moments_near[s, 0, :, columns].astype(F32),
                moments_near[s, 1, :, columns].astype(F32),
            )
            direction[32 * s : 32 * (s + 1), columns] = (
                m / bias_one / (jnp.sqrt(v / bias_two) + epsilon)
            ).astype(BF16)

    for n in range(8):
        back[q, :, 128 * n : 128 * (n + 1)] = lax.dot_general(
            direction[...],
            right_full[n],
            (((1,), (1,)), ((), ())),
            preferred_element_type=F32,
        ).astype(BF16)
    gather_back = RowGather(back)
    rotated_recv, rotated_sent = to_owners(rotated_out, rotated_in, rotated_in)
    gather_back.pass_on()
    gather_back.share()

    rotated_recv()

    @pl.loop(0, 4)
    def _(i):
        m, v = moments(clip_scale * rotated_in[i].astype(F32), first_in[i], second_in[i])
        new_first[i] = m
        new_second[i] = v

    gather_back.share_far()
    gather_back.finish()
    master_recv()

    def piece(a, b):
        return weights.at[jnp.where(is_x, b, a), 2 * jnp.where(is_x, a, b) + c]

    keep = 1.0 - learning_rate * decay_rate
    for n in range(4):
        columns = slice(256 * n, 256 * (n + 1))
        acc = jnp.dot(
            left_rows[...],
            back[:, :, columns].reshape(1024, 256),
            preferred_element_type=F32,
        )
        for s in range(4):
            rows = acc[32 * s : 32 * (s + 1)]
            update_out[s, :, columns] = rows.astype(BF16)
            weights[y, q, 32 * s : 32 * (s + 1), columns] = (
                master_near[s, :, columns].astype(F32) * keep - learning_rate * rows
            ).astype(BF16)

    pair = []

    def to_pair(ref):
        pair.append(message(ref, ref, partner))

    def spread(ref, there, back_there):
        up = [message(half(ref, 0), half(ref, 0), there)]
        down = [message(half(ref, 1), half(ref, 1), back_there)]
        up.append(message(half(ref, 1), half(ref, 1), there))
        down.append(message(half(ref, 0), half(ref, 0), back_there))
        return up, down

    a_legs = []

    def spread_a(b):
        got = piece(p_a, b)
        a_legs.append((b, *spread(got, at_a(1), at_a(-1))))
        to_pair(got)

    mine = piece(p_a, p_b)
    b_up, b_down = spread(mine, at_b(1), at_b(-1))
    spread_a(p_b)
    update_recv, update_sent = to_owners(update_out, update_in, update_in)

    def relay(prev, following, up, down, there, back_there):
        up[0].wait_recv()
        far_0 = message(half(prev, 0), half(prev, 0), there)
        down[0].wait_recv()
        far_1 = message(half(following, 1), half(following, 1), back_there)
        return far_0, far_1

    b_prev, b_next, b_far = [plus(p_b, d) for d in (-1, 1, 2)]
    b_fars = relay(piece(p_a, b_prev), piece(p_a, b_next), b_up, b_down, at_b(1), at_b(-1))
    fars = []

    def relay_a(n):
        b, up, down = a_legs[n]
        fars.append(
            relay(piece(a_prev, b), piece(a_next, b), up, down, at_a(1), at_a(-1))
        )

    def share_a(n):
        b, up, down = a_legs[n]
        up[1].wait_recv()
        to_pair(piece(a_prev, b))
        down[1].wait_recv()
        to_pair(piece(a_next, b))

    def share_far_a(n):
        far_0, far_1 = fars[n]
        got = piece(a_far, a_legs[n][0])
        far_0.wait_recv()
        to_pair(half(got, 0))
        far_1.wait_recv()
        to_pair(half(got, 1))

    relay_a(0)
    b_up[1].wait_recv()
    spread_a(b_prev)
    b_down[1].wait_recv()
    spread_a(b_next)
    share_a(0)
    b_fars[0].wait_recv()
    b_fars[1].wait_recv()
    spread_a(b_far)
    update_recv()

    @pl.loop(0, 4)
    def _(i):
        new_master[i] = master_in[i] * keep - learning_rate * update_in[i].astype(F32)

    relay_a(1)
    share_far_a(0)
    share_a(1)
    relay_a(2)
    share_far_a(1)
    share_a(2)
    relay_a(3)
    share_far_a(2)
    share_a(3)
    share_far_a(3)
    for copy in pair:
        copy.wait_recv()

    for copy in sent:
        copy.wait_send()
    for m in range(7):
        swap_copy(m, False).wait_send()
    right_sent()
    left_sent()
    moments_sent()
    master_sent()
    rotated_sent()
    update_sent()


def write_kernel(a, b, c, d, a_out, b_out, c_out, d_out, sems):
    copies = [pltpu.make_async_copy(a.at[i], a_out.at[i], sems.at[i]) for i in range(4)]
    for n, (source, place) in enumerate(((b, b_out), (c, c_out), (d, d_out))):
        copies.append(pltpu.make_async_copy(source, place, sems.at[4 + n]))
    for copy in copies:
        copy.start()
    for copy in copies:
        copy.wait()


def per_device(grad_parts, master, first_moment, second_moment, left_basis, right_basis):
    vmem = pl.BlockSpec(memory_space=pltpu.VMEM)
    hbm = pl.BlockSpec(memory_space=pltpu.HBM)
    state = pltpu.VMEM((4, 32, 1024), F32)
    outputs = pl.pallas_call(
        kernel,
        out_shape=(
            pltpu.VMEM((4, 8, 128, 1024), BF16),
            state,
            state,
            state,
        ),
        in_specs=[hbm] * 6,
        out_specs=(vmem, vmem, vmem, vmem),
        scratch_shapes=[
            pltpu.VMEM((4, 4, 128, 1024), BF16),
            pltpu.VMEM((4, 4, 128, 1024), BF16),
            pltpu.VMEM((6, 4, 64, 1024), BF16),
            pltpu.VMEM((6, 64, 1024), BF16),
            pltpu.VMEM((8, 128, 1024), BF16),
            pltpu.VMEM((128, 1024), BF16),
            pltpu.VMEM((8, 128, 128), BF16),
            pltpu.VMEM((8, 128, 1024), BF16),
            pltpu.VMEM((8, 128, 1024), BF16),
            pltpu.VMEM((4, 2, 32, 1024), BF16),
            pltpu.VMEM((4, 2, 32, 1024), BF16),
            pltpu.VMEM((4, 32, 1024), BF16),
            pltpu.VMEM((4, 32, 1024), BF16),
            pltpu.VMEM((4, 32, 1024), F32),
            pltpu.VMEM((4, 32, 1024), F32),
            pltpu.VMEM((4, 32, 1024), F32),
            pltpu.VMEM((128, 1024), BF16),
            pltpu.VMEM((128, 1024), BF16),
            pltpu.VMEM((4, 32, 1024), BF16),
            pltpu.VMEM((4, 32, 1024), BF16),
            pltpu.VMEM((4, 32, 1024), BF16),
            pltpu.VMEM((4, 32, 1024), BF16),
            pltpu.VMEM((16, 8, 128), F32),
            pltpu.SemaphoreType.DMA((N_SEMS,)),
            pltpu.SemaphoreType.DMA((N_SEMS,)),
            pltpu.SemaphoreType.DMA((11,)),
        ],
        compiler_params=pltpu.CompilerParams(
            collective_id=0, has_side_effects=True, vmem_limit_bytes=32 * 1024 * 1024
        ),
    )(
        *(
            pltpu.with_memory_space_constraint(array, pltpu.HBM)
            for array in (
                grad_parts.reshape(4, 4, 2, 128, 1024),
                master,
                first_moment,
                second_moment,
                left_basis,
                right_basis,
            )
        )
    )
    state = jax.ShapeDtypeStruct((4, 32, 1024), F32)
    weights, new_master, new_first, new_second = pl.pallas_call(
        write_kernel,
        out_shape=(jax.ShapeDtypeStruct((4, 8, 128, 1024), BF16), state, state, state),
        in_specs=[vmem] * 4,
        out_specs=(hbm, hbm, hbm, hbm),
        scratch_shapes=[pltpu.SemaphoreType.DMA((7,))],
        compiler_params=pltpu.CompilerParams(vmem_limit_bytes=4 * 1024 * 1024),
    )(*(pltpu.with_memory_space_constraint(array, pltpu.VMEM) for array in outputs))
    return (weights.reshape(4, 1024, 1024), new_master, new_first, new_second)


def solution(mesh):
    finer = Mesh(mesh.devices.reshape(4, 4, 2, mesh.shape["mp"]), ("dp_0", "dp_1", "dp_2", "mp"))
    placed = (
        P(DP, None, None, "mp"),
        P(None, DP, "mp"),
        P(None, DP, "mp"),
        P(None, DP, "mp"),
        P(None, DP, "mp"),
        P(None, DP, "mp"),
    )
    return jax.shard_map(
        per_device,
        mesh=finer,
        in_specs=placed,
        out_specs=(P(None, None, "mp"), P(None, DP, "mp"), P(None, DP, "mp"), P(None, DP, "mp")),
        check_vma=False,
    )
```

```python
import math

import jax
import jax.numpy as jnp
from jax import lax
from jax.experimental import pallas as pl
from jax.experimental.pallas import tpu as pltpu
from jax.sharding import Mesh
from jax.sharding import PartitionSpec as P

D = 4096
STEP = 10
DP = ("dp_0", "dp_1", "dp_2")
MESH = pl.DeviceIdType.MESH

beta_one = 0.95
beta_two = 0.95
epsilon = 1e-08
norm_epsilon = 1e-06
learning_rate = 0.3
decay_rate = 0.1

F32 = jnp.float32
BF16 = jnp.bfloat16
N_SENDS = 24
N_ARRIVALS = 70


def kernel(
    grad,
    master,
    first,
    second,
    left,
    right,
    weights,
    new_master,
    new_first,
    new_second,
    own,
    par,
    rec_a,
    rec_b,
    right_full,
    left_rows,
    left_cols,
    turned,
    back,
    moments_near,
    moments_out,
    master_near,
    master_out,
    master_in,
    first_in,
    second_in,
    grad_low,
    direction,
    rotated_out,
    rotated_in,
    sums,
    squares,
    send_sems,
    recv_sems,
    local_sems,
):
    x, y, c, z = [lax.axis_index(n) for n in ("dp_0", "dp_1", "dp_2", "mp")]
    is_x = c == 0
    p_a = jnp.where(is_x, x, y)
    p_b = jnp.where(is_x, y, x)
    q = 2 * x + c
    h_own = y // 2

    def plus(v, d):
        return lax.rem(v + (d % 4), 4)

    def at_a(d):
        return (jnp.where(is_x, plus(x, d), x), jnp.where(is_x, y, plus(y, d)), c, z)

    def at_b(d):
        return (jnp.where(is_x, x, plus(x, d)), jnp.where(is_x, plus(y, d), y), c, z)

    def at_x(d):
        return (plus(x, d), y, c, z)

    partner = (x, y, 1 - c, z)
    used_send, used_recv = [0], [0]

    def next_index(used):
        used[0] += 1
        return used[0] - 1

    def bytes_of(ref):
        return math.prod(ref.shape) * (4 if ref.dtype == F32 else 2)

    def wait_bytes(total, sem):
        rows, pieces = total // 2048, total // (256 * 1024)
        if rows < 32:
            ref = squares.at[pl.ds(0, total // 4096)]
        elif rows <= 128:
            ref = right_full.at[0, pl.ds(0, rows)]
        elif rows % 128 == 0 and pieces <= 8:
            ref = right_full.at[pl.ds(0, pieces)]
        elif rows % 64 == 0 and rows <= 512:
            ref = right_full.at[pl.ds(0, rows // 64), pl.ds(0, 64)]
        else:
            ref = own.at[pl.ds(0, pieces // 4)]
        assert bytes_of(ref) == total, total
        pltpu.make_async_copy(ref, ref, sem).wait()

    class Arrivals:
        def __init__(self):
            self.index = next_index(used_recv)
            self.total = 0

        def wait_recv(self):
            wait_bytes(self.total, recv_sems.at[self.index])

    send_lots = {}

    def send_index(size):
        lots = send_lots.setdefault(size, [])
        if not lots or lots[-1][1] == 8:
            lots.append([next_index(used_send), 0])
        lots[-1][1] += 1
        return lots[-1][0]

    def message(src, dst, device, arrivals=None):
        arrivals = Arrivals() if arrivals is None else arrivals
        arrivals.total += bytes_of(src)
        pltpu.make_async_remote_copy(
            src_ref=src,
            dst_ref=dst,
            send_sem=send_sems.at[send_index(bytes_of(src))],
            recv_sem=recv_sems.at[arrivals.index],
            device_id=device,
            device_id_type=MESH,
        ).start()
        return arrivals

    order_a = (2, 1, 3, 0)
    k_swap = [next_index(used_recv) for _ in range(7)]
    swap_sent = [next_index(used_send) for _ in range(2)]
    blocks = [(0, k) for k in range(4)] + [(n, None) for n in (1, 2, 3)]

    def source_of(n, k, of_x):
        a = plus(x if of_x else y, order_a[n])
        if k is None:
            return (grad.at[:, a, 0] if of_x else grad.at[a, :, 1]), (a,)
        b = plus(y if of_x else x, order_a[k])
        return (grad.at[b, a, 0] if of_x else grad.at[a, b, 1]), (a, b)

    def swap_copy(m, of_x):
        source, place = source_of(*blocks[m], of_x)
        return pltpu.make_async_remote_copy(
            src_ref=source,
            dst_ref=par.at[place],
            send_sem=send_sems.at[swap_sent[m // 4]],
            recv_sem=recv_sems.at[k_swap[m]],
            device_id=partner,
            device_id_type=MESH,
        )

    for m in range(7):
        for of_x in (True, False):

            @pl.when(is_x == of_x)
            def _():
                source, place = source_of(*blocks[m], of_x)
                pltpu.make_async_copy(source, own.at[place], local_sems.at[m]).start()

    for n, (source, place) in enumerate(
        ((first, first_in), (second, second_in), (master, master_in))
    ):
        pltpu.make_async_copy(source, place, local_sems.at[7 + n]).start()

    barrier = pltpu.get_barrier_semaphore()
    peers = [partner]
    for d in range(1, 4):
        peers += [(plus(x, d), y, c, z), (plus(x, d), y, 1 - c, z)]
        peers += [(x, plus(y, d), c, z), (x, plus(y, d), 1 - c, z)]
        peers += [(x, y, c, plus(z, d))]
    for device in peers:
        pl.semaphore_signal(barrier, inc=1, device_id=device, device_id_type=MESH)
    pl.semaphore_wait(barrier, len(peers))

    for m in range(7):
        for of_x in (True, False):

            @pl.when(is_x != of_x)
            def _():
                swap_copy(m, of_x).start()

    def wait_part(m):
        n, k = blocks[m]
        a = plus(p_a, order_a[n])
        place = (a,) if k is None else (a, plus(p_b, order_a[k]))
        pltpu.make_async_copy(own.at[place], own.at[place], local_sems.at[m]).wait()
        pltpu.make_async_copy(par.at[place], par.at[place], recv_sems.at[k_swap[m]]).wait()

    def add_part(a, b):
        @pl.loop(0, 4)
        def _(t):
            rows = pl.ds(pl.multiple_of(t * 32, 32), 32)
            own[a, b, rows, :] = own[a, b, rows, :] + par[a, b, rows, :]

    strip = 2 * lax.rem(y, 2) + c

    def wait_sent(one_stays, size, index):
        def wait_send():
            for copies, condition in ((3, one_stays), (4, jnp.logical_not(one_stays))):

                @pl.when(condition)
                def _():
                    wait_bytes(copies * size, send_sems.at[index])

        return wait_send

    def to_block(source, place, whole):
        arrived, left_here = next_index(used_recv), next_index(used_send)
        for i in range(4):
            self_case = jnp.logical_and(y == i, c == h_own)

            @pl.when(self_case)
            def _():
                pltpu.make_async_copy(source(i), place, recv_sems.at[arrived]).start()

            @pl.when(jnp.logical_not(self_case))
            def _():
                pltpu.make_async_remote_copy(
                    src_ref=source(i),
                    dst_ref=place,
                    send_sem=send_sems.at[left_here],
                    recv_sem=recv_sems.at[arrived],
                    device_id=(x, jnp.int32(i), h_own, z),
                    device_id_type=MESH,
                ).start()

        def wait_recv():
            pltpu.make_async_copy(whole, whole, recv_sems.at[arrived]).wait()

        return wait_recv, wait_sent(c == h_own, bytes_of(place), left_here)

    place_rows = pl.ds(pl.multiple_of(strip * 32, 32), 32)
    right_recv, right_sent = to_block(
        lambda i: right.at[i], right_full.at[2 * x + h_own, place_rows], right_full.at[q]
    )
    left_recv, left_sent = to_block(lambda i: left.at[i], left_rows.at[place_rows], left_rows)

    def to_owners(source, place, whole):
        arrived, left_here = next_index(used_recv), next_index(used_send)
        for s in range(4):
            yy, cc = 2 * c + s // 2, s % 2
            self_case = jnp.logical_and(yy == y, c == cc)

            @pl.when(self_case)
            def _():
                pltpu.make_async_copy(
                    source.at[s], place.at[y], recv_sems.at[arrived]
                ).start()

            @pl.when(jnp.logical_not(self_case))
            def _():
                pltpu.make_async_remote_copy(
                    src_ref=source.at[s],
                    dst_ref=place.at[y],
                    send_sem=send_sems.at[left_here],
                    recv_sem=recv_sems.at[arrived],
                    device_id=(x, yy, jnp.int32(cc), z),
                    device_id_type=MESH,
                ).start()

        def wait_recv():
            pltpu.make_async_copy(whole, whole, recv_sems.at[arrived]).wait()

        return wait_recv, wait_sent(y // 2 == c, bytes_of(source.at[0]), left_here)

    def half(ref, h):
        return ref.at[pl.ds(64 * h, 64)]

    class RowGather:
        def __init__(self, buf):
            self.left = buf.at[2 * plus(x, -1) + c]
            self.right = buf.at[2 * plus(x, 1) + c]
            self.far = buf.at[2 * plus(x, 2) + c]
            mine = buf.at[q]
            self.from_left = message(half(mine, 0), half(mine, 0), at_x(1))
            self.from_right = message(half(mine, 1), half(mine, 1), at_x(-1))
            self.rest = message(half(mine, 1), half(mine, 1), at_x(1))
            message(half(mine, 0), half(mine, 0), at_x(-1), self.rest)
            self.pair = message(mine, mine, partner)

        def pass_on(self):
            self.from_left.wait_recv()
            self.far_half = message(half(self.left, 0), half(self.left, 0), at_x(1))
            self.from_right.wait_recv()
            message(half(self.right, 1), half(self.right, 1), at_x(-1), self.far_half)

        def share(self):
            self.rest.wait_recv()
            message(self.left, self.left, partner, self.pair)
            message(self.right, self.right, partner, self.pair)

        def share_far(self):
            self.far_half.wait_recv()
            self.pair_far = message(self.far, self.far, partner)

    b_of = [plus(p_b, d) for d in order_a]
    halves = (pl.ds(0, 64), pl.ds(64, 64))

    a_far, a_next, a_prev, a_own = [plus(p_a, d) for d in order_a]
    relay_r, relay_l = [], []
    first_parts = [Arrivals() for _ in range(4)]
    for k in range(4):
        wait_part(k)
        add_part(a_far, b_of[k])
        relay_r.append(message(own.at[a_far, b_of[k], halves[0]], rec_a.at[0, k], at_a(1)))
        relay_l.append(message(own.at[a_far, b_of[k], halves[1]], rec_a.at[1, k], at_a(-1)))
    right_recv()
    gather_right = RowGather(right_full)
    wait_part(4)
    for k in range(4):
        add_part(a_next, b_of[k])
        message(own.at[a_next, b_of[k], halves[1]], rec_a.at[2, k], at_a(1), first_parts[k])
    wait_part(5)
    for k in range(4):
        add_part(a_prev, b_of[k])
        message(own.at[a_prev, b_of[k], halves[0]], rec_a.at[3, k], at_a(-1), first_parts[k])
    left_recv()
    mine = left_cols.at[q]
    tiles = Arrivals()
    for d in range(4):
        for e in range(2):
            xx, cc = plus(x, d), lax.rem(c + e, 2)
            columns = pl.ds(pl.multiple_of((2 * xx + cc) * 128, 128), 128)
            if d or e:
                message(left_rows.at[:, columns], mine, (xx, y, cc, z), tiles)
            else:
                own_tile = pltpu.make_async_copy(
                    left_rows.at[:, columns], mine, local_sems.at[10]
                )
                own_tile.start()

    wait_part(6)
    for k in range(4):
        add_part(a_own, b_of[k])

    for k in range(4):
        relay_r[k].wait_recv()
        own[a_next, b_of[k], 0:64, :] = own[a_next, b_of[k], 0:64, :] + rec_a[0, k]
        message(own.at[a_next, b_of[k], halves[0]], rec_a.at[4, k], at_a(1), first_parts[k])
        relay_l[k].wait_recv()
        own[a_prev, b_of[k], 64:128, :] = own[a_prev, b_of[k], 64:128, :] + rec_a[1, k]
        message(own.at[a_prev, b_of[k], halves[1]], rec_a.at[5, k], at_a(-1), first_parts[k])

    gather_right.pass_on()
    gather_right.share()

    for n, (ref, packed, m) in enumerate(
        ((first_in, moments_out, 0), (second_in, moments_out, 1), (master_in, master_out, None))
    ):
        pltpu.make_async_copy(ref, ref, local_sems.at[7 + n]).wait()

        @pl.loop(0, 4)
        def _(i):
            if m is None:
                packed[i] = ref[i].astype(BF16)
            else:
                packed[i, m] = ref[i].astype(BF16)

    moments_recv, moments_sent = to_block(
        lambda i: moments_out.at[i], moments_near.at[strip], moments_near
    )
    def sum_first(k):
        first_parts[k].wait_recv()
        own[a_own, b_of[k], 0:64, :] = (
            own[a_own, b_of[k], 0:64, :].astype(F32)
            + rec_a[3, k].astype(F32)
            + rec_a[4, k].astype(F32)
        ).astype(BF16)
        own[a_own, b_of[k], 64:128, :] = (
            own[a_own, b_of[k], 64:128, :].astype(F32)
            + rec_a[2, k].astype(F32)
            + rec_a[5, k].astype(F32)
        ).astype(BF16)

    sum_first(0)
    far = own.at[a_own, b_of[0]]
    second_relay_r = message(half(far, 0), rec_b.at[0], at_b(1))
    second_relay_l = message(half(far, 1), rec_b.at[1], at_b(-1))
    sum_first(1)
    second_parts = message(half(own.at[a_own, b_of[1]], 1), rec_b.at[2], at_b(1))
    sum_first(2)
    message(half(own.at[a_own, b_of[2]], 0), rec_b.at[3], at_b(-1), second_parts)
    second_relay_r.wait_recv()
    own[a_own, b_of[1], 0:64, :] = own[a_own, b_of[1], 0:64, :] + rec_b[0]
    message(half(own.at[a_own, b_of[1]], 0), rec_b.at[4], at_b(1), second_parts)
    second_relay_l.wait_recv()
    own[a_own, b_of[2], 64:128, :] = own[a_own, b_of[2], 64:128, :] + rec_b[1]
    message(half(own.at[a_own, b_of[2]], 1), rec_b.at[5], at_b(-1), second_parts)
    sum_first(3)
    gather_right.share_far()

    def sum_second(rows, one, two):
        total = jnp.zeros((8, 1024), F32)
        for r in range(0, 64, 16):
            at = pl.ds(rows + r, 16)
            part = pl.ds(r, 16)
            value = (
                own[a_own, p_b, at, :].astype(F32)
                + rec_b[one, part, :].astype(F32)
                + rec_b[two, part, :].astype(F32)
            )
            grad_low[at, :] = value.astype(BF16)
            total = total + (value * value).reshape(2, 8, 1024).sum(0)
        return total

    second_parts.wait_recv()
    total = sum_second(0, 3, 4) + sum_second(64, 2, 5)
    squares[0] = sum(total[:, 128 * k : 128 * (k + 1)] for k in range(8))
    over_row = message(squares.at[0], squares.at[1], partner)
    for d in (1, 2, 3):
        for n, cc in enumerate((c, 1 - c)):
            place = squares.at[2 * d + n]
            message(squares.at[0], place, (plus(x, d), y, cc, z), over_row)

    gather_right.pair.wait_recv()
    gather_right.pair_far.wait_recv()
    for n in range(4):
        columns = slice(256 * n, 256 * (n + 1))
        acc = jnp.zeros((128, 256), F32)
        for k in range(8):
            acc = acc + jnp.dot(
                grad_low[:, 128 * k : 128 * (k + 1)],
                right_full[k, :, columns],
                preferred_element_type=F32,
            )
        turned[q, :, columns] = acc.astype(BF16)
    gather_turned = RowGather(turned)
    over_row.wait_recv()
    squares[8] = sum(squares[n] for n in range(8))
    over_y, over_z = Arrivals(), Arrivals()
    for d in (1, 2, 3):
        message(squares.at[8], squares.at[8 + d], (x, plus(y, d), c, z), over_y)
    master_recv, master_sent = to_block(
        lambda i: master_out.at[i], master_near.at[strip], master_near
    )
    gather_turned.pass_on()
    over_y.wait_recv()
    squares[12] = sum(squares[n] for n in range(8, 12))
    for d in (1, 2, 3):
        message(squares.at[12], squares.at[12 + d], (x, y, c, plus(z, d)), over_z)
    gather_turned.share()
    own_tile.wait()
    tiles.wait_recv()
    gather_turned.pair.wait_recv()

    def rotated_from(chip, columns):
        pieces = pl.ds(2 * chip, 2)
        return lax.dot_general(
            left_cols[pieces].reshape(256, 128),
            turned[pieces, :, columns].reshape(256, 256),
            (((0,), (0,)), ((), ())),
            preferred_element_type=F32,
        )

    near = (x, plus(x, -1), plus(x, 1))
    for n in range(4):
        columns = slice(256 * n, 256 * (n + 1))
        sums[:, columns] = sum(rotated_from(chip, columns) for chip in near)
    gather_turned.share_far()
    over_z.wait_recv()
    total = sum(squares[n] for n in range(12, 16))
    squares_sum = jnp.sum(jnp.sum(total, axis=1, keepdims=True), axis=0, keepdims=True)
    clip_scale = jnp.minimum(1.0, 2.0 * D / jnp.sqrt(squares_sum + norm_epsilon))

    moments_recv()
    gather_turned.pair_far.wait_recv()
    bias_one = 1.0 - beta_one**STEP
    bias_two = 1.0 - beta_two**STEP

    def moments(clipped, m, v):
        return (
            beta_one * m + (1.0 - beta_one) * clipped,
            beta_two * v + (1.0 - beta_two) * clipped * clipped,
        )

    for n in range(4):
        columns = slice(256 * n, 256 * (n + 1))
        acc = sums[:, columns] + rotated_from(plus(x, 2), columns)
        for s in range(4):
            rows = acc[32 * s : 32 * (s + 1)]
            rotated_out[s, :, columns] = rows.astype(BF16)
            m, v = moments(
                clip_scale * rows,
                moments_near[s, 0, :, columns].astype(F32),
                moments_near[s, 1, :, columns].astype(F32),
            )
            direction[32 * s : 32 * (s + 1), columns] = (
                m / bias_one / (jnp.sqrt(v / bias_two) + epsilon)
            ).astype(BF16)

    for n in range(8):
        back[q, :, 128 * n : 128 * (n + 1)] = lax.dot_general(
            direction[...],
            right_full[n],
            (((1,), (1,)), ((), ())),
            preferred_element_type=F32,
        ).astype(BF16)
    gather_back = RowGather(back)
    rotated_recv, rotated_sent = to_owners(rotated_out, rotated_in, rotated_in)
    gather_back.pass_on()
    gather_back.share()

    rotated_recv()

    @pl.loop(0, 4)
    def _(i):
        m, v = moments(clip_scale * rotated_in[i].astype(F32), first_in[i], second_in[i])
        new_first[i] = m
        new_second[i] = v

    def update_from(chip, columns):
        pieces = pl.ds(2 * chip, 2)
        return jnp.dot(
            left_rows[:, pl.ds(pl.multiple_of(256 * chip, 256), 256)],
            back[pieces, :, columns].reshape(256, 256),
            preferred_element_type=F32,
        )

    master_recv()
    gather_back.pair.wait_recv()
    for n in range(4):
        columns = slice(256 * n, 256 * (n + 1))
        sums[:, columns] = sum(update_from(chip, columns) for chip in near)
    gather_back.share_far()
    gather_back.pair_far.wait_recv()

    def piece(a, b):
        return weights.at[jnp.where(is_x, b, a), 2 * jnp.where(is_x, a, b) + c]

    keep = 1.0 - learning_rate * decay_rate
    for n in range(4):
        columns = slice(256 * n, 256 * (n + 1))
        acc = sums[:, columns] + update_from(plus(x, 2), columns)
        for s in range(4):
            rows = acc[32 * s : 32 * (s + 1)]
            weights[y, q, 32 * s : 32 * (s + 1), columns] = (
                master_near[s, :, columns].astype(F32) * keep - learning_rate * rows
            ).astype(BF16)

    pair = Arrivals()

    def to_pair(ref):
        message(ref, ref, partner, pair)

    class Ring:
        def __init__(self, piece_at, at):
            self.prev, self.following, self.far = [piece_at(d) for d in (-1, 1, 2)]
            self.at = at
            piece = piece_at(0)
            self.up = message(half(piece, 0), half(piece, 0), at(1))
            self.down = message(half(piece, 1), half(piece, 1), at(-1))
            self.rest = message(half(piece, 1), half(piece, 1), at(1))
            message(half(piece, 0), half(piece, 0), at(-1), self.rest)

        def relay(self):
            self.up.wait_recv()
            piece = half(self.prev, 0)
            self.far_halves = message(piece, piece, self.at(1))
            self.down.wait_recv()
            piece = half(self.following, 1)
            message(piece, piece, self.at(-1), self.far_halves)

    def along_a(b):
        return Ring(lambda d: piece(plus(p_a, d), b), at_a)

    def share(ring):
        ring.rest.wait_recv()
        to_pair(ring.prev)
        to_pair(ring.following)

    def share_far(ring):
        ring.far_halves.wait_recv()
        to_pair(ring.far)

    ring_b = Ring(lambda d: piece(p_a, plus(p_b, d)), at_b)
    rings = [along_a(p_b)]
    to_pair(piece(p_a, p_b))
    ring_b.relay()
    rings[0].relay()
    share(ring_b)
    rings += [along_a(plus(p_b, -1)), along_a(plus(p_b, 1))]
    share_far(ring_b)
    rings.append(along_a(plus(p_b, 2)))
    share(rings[0])
    for n in (1, 2, 3):
        rings[n].relay()
        share_far(rings[n - 1])
        share(rings[n])
    share_far(rings[3])
    pair.wait_recv()

    @pl.loop(0, 4)
    def _(i):
        old = master_in[i]
        low = old.astype(BF16).astype(F32)
        new_master[i] = weights[i, 2 * x + h_own, place_rows, :].astype(F32) + keep * (old - low)

    for size, lots in send_lots.items():
        for index, copies in lots:
            wait_bytes(size * copies, send_sems.at[index])
    wait_bytes(4 * 256 * 1024, send_sems.at[swap_sent[0]])
    wait_bytes(3 * 1024 * 1024, send_sems.at[swap_sent[1]])
    right_sent()
    left_sent()
    moments_sent()
    master_sent()
    rotated_sent()
    assert used_send[0] <= N_SENDS and used_recv[0] <= N_ARRIVALS, (used_send, used_recv)


def write_kernel(a, b, c, d, a_out, b_out, c_out, d_out, sems):
    copies = [
        pltpu.make_async_copy(
            a.at[i, pl.ds(4 * j, 4)], a_out.at[i, pl.ds(4 * j, 4)], sems.at[2 * i + j]
        )
        for i in range(4)
        for j in range(2)
    ]
    for n, (source, place) in enumerate(((b, b_out), (c, c_out), (d, d_out))):
        copies.append(pltpu.make_async_copy(source, place, sems.at[8 + n]))
    for copy in copies:
        copy.start()
    for copy in copies:
        copy.wait()


def per_device(grad_parts, master, first_moment, second_moment, left_basis, right_basis):
    vmem = pl.BlockSpec(memory_space=pltpu.VMEM)
    hbm = pl.BlockSpec(memory_space=pltpu.HBM)
    state = pltpu.VMEM((4, 32, 1024), F32)
    outputs = pl.pallas_call(
        kernel,
        out_shape=(
            pltpu.VMEM((4, 8, 128, 1024), BF16),
            state,
            state,
            state,
        ),
        in_specs=[hbm] * 6,
        out_specs=(vmem, vmem, vmem, vmem),
        scratch_shapes=[
            pltpu.VMEM((4, 4, 128, 1024), BF16),
            pltpu.VMEM((4, 4, 128, 1024), BF16),
            pltpu.VMEM((6, 4, 64, 1024), BF16),
            pltpu.VMEM((6, 64, 1024), BF16),
            pltpu.VMEM((8, 128, 1024), BF16),
            pltpu.VMEM((128, 1024), BF16),
            pltpu.VMEM((8, 128, 128), BF16),
            pltpu.VMEM((8, 128, 1024), BF16),
            pltpu.VMEM((8, 128, 1024), BF16),
            pltpu.VMEM((4, 2, 32, 1024), BF16),
            pltpu.VMEM((4, 2, 32, 1024), BF16),
            pltpu.VMEM((4, 32, 1024), BF16),
            pltpu.VMEM((4, 32, 1024), BF16),
            pltpu.VMEM((4, 32, 1024), F32),
            pltpu.VMEM((4, 32, 1024), F32),
            pltpu.VMEM((4, 32, 1024), F32),
            pltpu.VMEM((128, 1024), BF16),
            pltpu.VMEM((128, 1024), BF16),
            pltpu.VMEM((4, 32, 1024), BF16),
            pltpu.VMEM((4, 32, 1024), BF16),
            pltpu.VMEM((128, 1024), F32),
            pltpu.VMEM((16, 8, 128), F32),
            pltpu.SemaphoreType.DMA((N_SENDS,)),
            pltpu.SemaphoreType.DMA((N_ARRIVALS,)),
            pltpu.SemaphoreType.DMA((11,)),
        ],
        compiler_params=pltpu.CompilerParams(
            collective_id=0, has_side_effects=True, vmem_limit_bytes=32 * 1024 * 1024
        ),
    )(
        *(
            pltpu.with_memory_space_constraint(array, pltpu.HBM)
            for array in (
                grad_parts.reshape(4, 4, 2, 128, 1024),
                master,
                first_moment,
                second_moment,
                left_basis,
                right_basis,
            )
        )
    )
    state = jax.ShapeDtypeStruct((4, 32, 1024), F32)
    weights, new_master, new_first, new_second = pl.pallas_call(
        write_kernel,
        out_shape=(jax.ShapeDtypeStruct((4, 8, 128, 1024), BF16), state, state, state),
        in_specs=[vmem] * 4,
        out_specs=(hbm, hbm, hbm, hbm),
        scratch_shapes=[pltpu.SemaphoreType.DMA((11,))],
        compiler_params=pltpu.CompilerParams(vmem_limit_bytes=4 * 1024 * 1024),
    )(*(pltpu.with_memory_space_constraint(array, pltpu.VMEM) for array in outputs))
    return (weights.reshape(4, 1024, 1024), new_master, new_first, new_second)


def solution(mesh):
    finer = Mesh(mesh.devices.reshape(4, 4, 2, mesh.shape["mp"]), ("dp_0", "dp_1", "dp_2", "mp"))
    placed = (
        P(DP, None, None, "mp"),
        P(None, DP, "mp"),
        P(None, DP, "mp"),
        P(None, DP, "mp"),
        P(None, DP, "mp"),
        P(None, DP, "mp"),
    )
    return jax.shard_map(
        per_device,
        mesh=finer,
        in_specs=placed,
        out_specs=(P(None, None, "mp"), P(None, DP, "mp"), P(None, DP, "mp"), P(None, DP, "mp")),
        check_vma=False,
    )
```
